512 devices in a mesh: frame: 32 (over x, z), feat: 16 (over y, core).
Axes of the slice: x: 4, y: 8, z: 8, core: 2. Of those that a mesh axis runs over, the one named last changes fastest.
Arguments:
- coords: bfloat16 [32, 64, 3, 128], P('frame', 'feat'), may hold values from -9 to 9
- walker_map: int32 [32, 64], P('frame', 'feat'), may hold values from 0 to 63, each once within a row
- pairs: int32 [2, 16384], P(None, 'feat'), may hold values from 0 to 127, as said below
Outputs:
- inst_cov: float32 [16384, 16384], P('feat', 'frame')
- lag_cov: float32 [16384, 16384], P('feat', 'frame')
The draws below stay inside these ranges and needn't reach their ends.
Inputs may be any that keep to these rules, and one draw needn't show every extreme that they name: `pairs`: the two blocks of a feature differ.
All inputs are finite; a program needn't handle non-finite values.
Results may differ from the reference program's by a relative error of at most 0.0038.
Values may be sent and summed in bfloat16 or wider, within the bound.
A program may use at most 64 MiB of HBM per device.

```python
import jax
import jax.numpy as jnp
from jax import lax

REPLICAS = 64
BLOCKS = 128
FEATURES = 16384
FRAMES = 32
LAG = 10


def draw_pairs(key, part):
    key_first, key_step = jax.random.split(jax.random.fold_in(key, 11))
    first = jax.random.randint(key_first, (FEATURES,), 0, BLOCKS)
    offset = jax.random.randint(key_step, (FEATURES,), 1, BLOCKS)
    second = (first + offset) % BLOCKS
    return jnp.stack([first, second]).astype(jnp.int32)


def block_levels(rng, extent, cuts, least, largest):
    def one(position, parts):
        heights = jax.random.uniform(jax.random.fold_in(jax.random.fold_in(rng, 6), position), (parts,), jnp.float32, least / len(cuts), largest / len(cuts))
        return jnp.repeat(jnp.exp(heights), extent[position] // parts).reshape((-1,) + (1,) * (len(extent) - position - 1))

    loudness = one(*cuts[0])
    for cut in cuts[1:]:
        loudness = loudness * one(*cut)
    return loudness


def noise(own_key, dims, scale, most, pieces=(), kind=jnp.bfloat16):
    entries = scale * jax.random.normal(own_key, dims, jnp.float32)
    if pieces:
        entries = entries * block_levels(own_key, dims, pieces, -0.22, 0.18)
    return jnp.clip(entries, -most, most).astype(kind)


def setup_inputs(seed: int = 0) -> dict:
    seeds = jax.random.split(jax.random.key(seed), 4)
    coords = noise(seeds[0], (FRAMES, REPLICAS, 3, BLOCKS), 1.5, 9.0, ((0, 32), (1, 16)))
    walker_map = jax.vmap(lambda own: jax.random.permutation(own, REPLICAS))(jax.random.split(seeds[1], FRAMES)).reshape((FRAMES, REPLICAS)).astype(jnp.int32)
    pairs = draw_pairs(jax.random.fold_in(seeds[3], 71), 0)
    return {"coords": coords, "walker_map": walker_map, "pairs": pairs}


def demux(coords, walker_map):
    count = walker_map.shape[1]
    labels = jnp.arange(count, dtype=jnp.int32)
    match = walker_map[:, :, None] == labels[None, None, :]
    inverse = lax.optimization_barrier(jnp.sum(jnp.where(match, labels[None, :, None], 0), axis=1)).astype(jnp.int32)
    return jnp.take_along_axis(coords, inverse[:, :, None, None], axis=1)

def reference(coords, walker_map, pairs):
    walker_coords = demux(coords, walker_map)

    def measure(frame_coords):
        values = frame_coords.astype(jnp.float32)
        diff = jnp.take(values, pairs[0], axis=-1) - jnp.take(values, pairs[1], axis=-1)
        return jnp.sqrt(lax.optimization_barrier(jnp.sum(diff * diff, axis=-2)))
    features = lax.map(measure, walker_coords)
    means = lax.optimization_barrier(jnp.mean(features, axis=(0, 1)))
    centered = (features - means).astype(jnp.bfloat16)
    flat = centered.reshape(-1, FEATURES)
    contract = (((0,), (0,)), ((), ()))
    inst_cov = lax.dot_general(flat, flat, contract, preferred_element_type=jnp.float32) / (FRAMES * REPLICAS)
    early = centered[:FRAMES - LAG].reshape(-1, FEATURES)
    late = centered[LAG:].reshape(-1, FEATURES)
    lag_cov = lax.dot_general(early, late, contract, preferred_element_type=jnp.float32) / ((FRAMES - LAG) * REPLICAS)
    return (inst_cov, lag_cov)
```

```python
import jax
import jax.numpy as jnp
from jax import lax
from jax.experimental import pallas as pl
from jax.experimental.pallas import tpu as pltpu
from jax.sharding import Mesh
from jax.sharding import PartitionSpec as P

F32, BF16, I32 = jnp.float32, jnp.bfloat16, jnp.int32
MESH = pl.DeviceIdType.MESH
NT = (((1,), (1,)), ((), ()))
TINY = 1e-37
X, Z, Y, C = 4, 8, 8, 2
FEAT = Y * C
BLOCKS = 128
FRAMES, REPLICAS, LAG = 32, 64, 10
ROWS, COLS = 1024, 512
GROUP = X * REPLICAS
SAMPLES = FRAMES * REPLICAS
PAIRED = (FRAMES - LAG) * REPLICAS
NEAR = (0, 1, 3, 2)


def gather_kernel(tile_ref, pairs_ref, g_ref, cp_ref, y_ref, s1, r1, sp, rp, sx, rx, su, sd, rg, sc, rc):
    x, z, y, c = (lax.axis_index(a) for a in ("x", "z", "y", "core"))
    me = y * C + c
    frame = x * Z + z
    owner = frame // 2

    def feat(k):
        f = lax.rem(me + k, FEAT)
        return {"y": f // C, "core": lax.rem(f, C)}

    def along_x(k):
        return {"x": lax.rem(x + k, X)}

    def along_z(k):
        return {"z": lax.rem(z + k + Z, Z)}

    other = {"core": 1 - c}

    barrier = pltpu.get_barrier_semaphore()
    for k in range(1, FEAT):
        pl.semaphore_signal(barrier, inc=1, device_id=feat(k), device_id_type=MESH)
    for k in range(1, X):
        pl.semaphore_signal(barrier, inc=1, device_id=along_x(k), device_id_type=MESH)
    for k in (1, -1):
        pl.semaphore_signal(barrier, inc=1, device_id=along_z(k), device_id_type=MESH)
    pl.semaphore_wait(barrier, FEAT - 1 + X - 1 + 2)

    def tile_copy(k, slot):
        return pltpu.make_async_remote_copy(
            src_ref=tile_ref, dst_ref=y_ref.at[slot], send_sem=s1.at[k], recv_sem=r1.at[slot],
            device_id=feat(k), device_id_type=MESH)

    for k in range(1, FEAT):
        tile_copy(k, me).start()

    def pair_copy(k):
        return pltpu.make_async_remote_copy(
            src_ref=pairs_ref.at[:, pl.ds(pl.multiple_of(lax.rem(frame, 2) * COLS, COLS), COLS)], dst_ref=cp_ref,
            send_sem=sp.at[k], recv_sem=rp, device_id=feat(k), device_id_type=MESH)

    @pl.when(me == owner)
    def _():
        for k in range(1, FEAT):
            pair_copy(k).start()
        cp_ref[...] = pairs_ref[:, pl.ds(pl.multiple_of(lax.rem(frame, 2) * COLS, COLS), COLS)]
        for k in range(1, FEAT):
            pair_copy(k).wait_send()

    @pl.when(me != owner)
    def _():
        pair_copy(1).wait_recv()

    y_ref[me] = tile_ref[...]
    for k in range(1, FEAT):
        tile_copy(k, lax.rem(me + k, FEAT)).wait_recv()

    tiles = y_ref[...]
    low = jnp.sum(tiles[:8].astype(F32), axis=0)[12:13]
    high = jnp.sum(tiles[8:].astype(F32), axis=0)[12:13]
    places = jnp.concatenate([low, high], axis=1)
    ids = lax.broadcasted_iota(I32, (192, 256), 0).astype(F32)
    match = (ids == places).astype(F32).astype(BF16)
    own = jnp.dot(match, tiles.reshape(256, BLOCKS), preferred_element_type=F32).astype(BF16)
    g_ref[0, z, x] = own[:96]
    g_ref[1, z, x] = own[96:]

    def x_copy(k, xx):
        return pltpu.make_async_remote_copy(
            src_ref=g_ref.at[c, z, x], dst_ref=g_ref.at[c, z, xx], send_sem=sx.at[k], recv_sem=rx.at[xx],
            device_id=along_x(k), device_id_type=MESH)

    def z_copy(step, zz, xx):
        return pltpu.make_async_remote_copy(
            src_ref=g_ref.at[c, zz, xx], dst_ref=g_ref.at[c, zz, xx],
            send_sem=(su if step > 0 else sd).at[zz, xx], recv_sem=rg.at[zz, xx],
            device_id=along_z(step), device_id_type=MESH)

    def core_copy(half, zz, xx):
        return pltpu.make_async_remote_copy(
            src_ref=g_ref.at[half, zz, xx], dst_ref=g_ref.at[half, zz, xx], send_sem=sc.at[zz, xx], recv_sem=rc.at[zz, xx],
            device_id=other, device_id_type=MESH)

    for k in range(1, X):
        x_copy(k, x).start()
    xs = [lax.rem(x + k, X) for k in NEAR]
    for n, xx in enumerate(xs):
        if n:
            x_copy(1, xx).wait_recv()
        z_copy(1, z, xx).start()
        z_copy(-1, z, xx).start()
        if n:
            core_copy(c, z, xx).start()
    for s in range(1, 5):
        for sign in (1, -1):
            zz = lax.rem(z - sign * s + Z, Z)
            for n, xx in enumerate(xs):
                if s == 4 and (n < 2) != (sign > 0):
                    continue
                z_copy(sign, zz, xx).wait_recv()
                if s < 3 or (s == 3 and (n < 2) == (sign > 0)):
                    z_copy(sign, zz, xx).start()
                core_copy(c, zz, xx).start()

    for s in range(0, 5):
        for sign in (1, -1):
            zz = lax.rem(z - sign * s + Z, Z)
            for n, xx in enumerate(xs):
                if (s == 0 and (n == 0 or sign < 0)) or (s == 4 and (n < 2) != (sign > 0)):
                    continue
                core_copy(1 - c, zz, xx).wait_recv()
                core_copy(c, zz, xx).wait_send()
    for k in range(1, FEAT):
        tile_copy(k, me).wait_send()
    for k in range(1, X):
        x_copy(k, x).wait_send()
    for s in range(0, 4):
        for sign in (1, -1):
            zz = lax.rem(z - sign * s + Z, Z)
            for n, xx in enumerate(xs):
                if s < 3 or (n < 2) == (sign > 0):
                    z_copy(sign, zz, xx).wait_send()


def gather(tile, pairs):
    vmem = pl.BlockSpec(memory_space=pltpu.VMEM)
    dma = pltpu.SemaphoreType.DMA
    return pl.pallas_call(
        gather_kernel,
        out_shape=(
            jax.ShapeDtypeStruct((C, Z, X, 96, BLOCKS), BF16),
            jax.ShapeDtypeStruct((2, COLS), I32),
        ),
        in_specs=[vmem, vmem],
        out_specs=(vmem, vmem),
        scratch_shapes=[
            pltpu.VMEM((FEAT, 16, BLOCKS), BF16),
            dma((FEAT,)), dma((FEAT,)), dma((FEAT,)), dma, dma((X,)), dma((X,)),
            dma((Z, X)), dma((Z, X)), dma((Z, X)), dma((Z, X)), dma((Z, X)),
        ],
        compiler_params=pltpu.CompilerParams(collective_id=0, has_side_effects=True, vmem_limit_bytes=16 << 20),
        name="gather",
    )(tile, pairs)


def root(s):
    return s * lax.rsqrt(jnp.maximum(s, TINY))


def pair_matrix(pairs):
    ids = lax.broadcasted_iota(I32, (BLOCKS, pairs.shape[1]), 0)
    return (ids == pairs[0:1]).astype(F32) - (ids == pairs[1:2]).astype(F32)


def covariance_kernel(
    g_ref, rp_ref, cp_ref, inst_ref, lag_ref,
    left_pairs, right_pairs, left_raw, right_raw, left, right, left_sum, right_sum, inst, lag, sem,
):
    for j in range(ROWS // BLOCKS):
        part = pl.ds(j * BLOCKS, BLOCKS)
        left_pairs[part, :] = pair_matrix(rp_ref[:, part]).T.astype(BF16)
    right_pairs[...] = pair_matrix(cp_ref[...]).astype(BF16)
    left_sum[...] = jnp.zeros_like(left_sum)
    right_sum[...] = jnp.zeros_like(right_sum)

    @pl.loop(0, Z)
    def _(z):
        comps = [
            jnp.concatenate(
                [g_ref[h, z, x, k * 32 : (k + 1) * 32, :] for x in range(X) for h in range(C)], axis=0)
            for k in range(3)
        ]
        part = pl.ds(pl.multiple_of(z * GROUP, GROUP), GROUP)
        total = None
        for comp in comps:
            d = lax.dot_general(left_pairs[...], comp, NT, preferred_element_type=F32)
            total = d * d if total is None else total + d * d
        f = root(total)
        left_raw[:, part] = f
        left_sum[...] += f[:, :128] + f[:, 128:]
        total = None
        for comp in comps:
            d = jnp.dot(comp, right_pairs[...], preferred_element_type=F32)
            total = d * d if total is None else total + d * d
        f = root(total)
        right_raw[part, :] = f
        right_sum[...] += jnp.sum(f.reshape(GROUP // 8, 8, COLS), axis=0)

    left_mean = jnp.sum(left_sum[...], axis=1, keepdims=True) * (1.0 / SAMPLES)
    right_mean = jnp.sum(right_sum[...], axis=0, keepdims=True) * (1.0 / SAMPLES)
    for z in range(Z):
        part = pl.ds(z * GROUP, GROUP)
        left[:, part] = (left_raw[:, part] - left_mean).astype(BF16)
        right[part, :] = (right_raw[part, :] - right_mean).astype(BF16)

    step = 256
    steps = ROWS // step

    def out_copies(k):
        rows = pl.ds(k * step, step)
        return (
            pltpu.make_async_copy(inst.at[rows], inst_ref.at[rows], sem.at[k]),
            pltpu.make_async_copy(lag.at[rows], lag_ref.at[rows], sem.at[steps + k]),
        )

    for k in range(steps):
        rows = pl.ds(k * step, step)
        inst[rows, :] = jnp.dot(left[rows, :], right[...], preferred_element_type=F32) * (1.0 / SAMPLES)
        out_copies(k)[0].start()
    for k in range(steps):
        rows = pl.ds(k * step, step)
        total = None
        for z in range(Z):
            if z + LAG - Z < Z:
                late = right[pl.ds((z + LAG - Z) * GROUP + REPLICAS, 3 * REPLICAS), :]
                late = jnp.concatenate([late, jnp.zeros((REPLICAS, COLS), BF16)], axis=0)
            else:
                late = right[pl.ds((z + LAG - 2 * Z) * GROUP + 2 * REPLICAS, 2 * REPLICAS), :]
            early = left[rows, pl.ds(z * GROUP, late.shape[0])]
            t = jnp.dot(early, late, preferred_element_type=F32)
            total = t if total is None else total + t
        lag[rows, :] = total * (1.0 / PAIRED)
        out_copies(k)[1].start()
    for k in range(steps):
        for copy in out_copies(k):
            copy.wait()


def covariances(g, row_pairs, col_pairs):
    vmem = pl.BlockSpec(memory_space=pltpu.VMEM)
    hbm = pl.BlockSpec(memory_space=pl.ANY)
    return pl.pallas_call(
        covariance_kernel,
        out_shape=(jax.ShapeDtypeStruct((ROWS, COLS), F32),) * 2,
        in_specs=[vmem] * 3,
        out_specs=(hbm, hbm),
        scratch_shapes=[
            pltpu.VMEM((ROWS, BLOCKS), BF16),
            pltpu.VMEM((BLOCKS, COLS), BF16),
            pltpu.VMEM((ROWS, SAMPLES), F32),
            pltpu.VMEM((SAMPLES, COLS), F32),
            pltpu.VMEM((ROWS, SAMPLES), BF16),
            pltpu.VMEM((SAMPLES, COLS), BF16),
            pltpu.VMEM((ROWS, 128), F32),
            pltpu.VMEM((8, COLS), F32),
            pltpu.VMEM((ROWS, COLS), F32),
            pltpu.VMEM((ROWS, COLS), F32),
            pltpu.SemaphoreType.DMA((8,)),
        ],
        compiler_params=pltpu.CompilerParams(vmem_limit_bytes=48 << 20),
        name="covariances",
    )(g, row_pairs, col_pairs)


def tile_of(coords, walker_map):
    count = coords.shape[1]
    rows = jnp.transpose(coords[0], (1, 0, 2)).reshape(3 * count, BLOCKS).astype(F32)
    device = lax.axis_index("y") * C + lax.axis_index("core")
    lane = lax.broadcasted_iota(I32, (1, BLOCKS), 1)
    j = lane - lax.rem(device, 8) * 16
    w = walker_map[0]
    place = (w // 32) * 96 + lax.rem(w, 32)
    here = jnp.full((1, BLOCKS), -1, I32)
    for i in range(count):
        here = jnp.where((j < 3 * count) & (lax.rem(j, count) == i), place[i] + (j // count) * 32, here)
    here = jnp.where((j >= 0) & (j < 16), here, 0)
    return jnp.concatenate([rows, here.astype(F32), jnp.zeros((3, BLOCKS), F32)], axis=0).astype(BF16)


def per_device(coords, walker_map, pairs):
    g, col_pairs = gather(tile_of(coords, walker_map), pairs)
    return covariances(g, pairs, col_pairs)


def solution(mesh):
    split = Mesh(mesh.devices.reshape(X, Z, Y, C), ("x", "z", "y", "core"))
    frame, feat = ("x", "z"), ("y", "core")
    return jax.shard_map(
        per_device,
        mesh=split,
        in_specs=(P(frame, feat, None, None), P(frame, feat), P(None, feat)),
        out_specs=(P(feat, frame), P(feat, frame)),
        check_vma=False,
    )
```

```python
import jax
import jax.numpy as jnp
from jax import lax
from jax.experimental import pallas as pl
from jax.experimental.pallas import tpu as pltpu
from jax.sharding import Mesh
from jax.sharding import PartitionSpec as P

F32, BF16, I32 = jnp.float32, jnp.bfloat16, jnp.int32
MESH = pl.DeviceIdType.MESH
NT = (((1,), (1,)), ((), ()))
TINY = 1e-37
X, Z, Y, C = 4, 8, 8, 2
FEAT = Y * C
BLOCKS = 128
FRAMES, REPLICAS, LAG = 32, 64, 10
HALF = REPLICAS // C
OWN = REPLICAS // FEAT
ROWS, COLS = 1024, 512
SPAN = 4
GROUP = SPAN * REPLICAS
SAMPLES = FRAMES * REPLICAS
PAIRED = (FRAMES - LAG) * REPLICAS
DISTANCES = (1, -1, 2, -2, 3, -3, 4)


def root(s):
    return s * lax.rsqrt(jnp.maximum(s, TINY))


def pair_matrix(pairs):
    ids = lax.broadcasted_iota(I32, (BLOCKS, pairs.shape[1]), 0)
    return (ids == pairs[0:1]).astype(F32) - (ids == pairs[1:2]).astype(F32)


def features_kernel(
    coords_hbm, map_hbm, pairs_hbm,
    left_ref, right_ref, left_sum, right_sum,
    coords_ref, map_ref, pairs_ref, wide_ref, tile_ref, y_ref, cp_ref, g_ref, left_pairs, right_pairs,
    sl, s1, r1, sp, rp, sz, rz, sx, rx, sc, rc,
):
    x, z, y, c = (lax.axis_index(a) for a in ("x", "z", "y", "core"))
    me = y * C + c
    frame = x * Z + z
    owner = frame // 2
    near = z // SPAN

    def feat(k):
        f = lax.rem(me + k, FEAT)
        return {"y": f // C, "core": lax.rem(f, C)}

    def along_x(k):
        return {"x": lax.rem(x + k, X)}

    def along_z(k):
        return {"z": lax.rem(z + k + Z, Z)}

    barrier = pltpu.get_barrier_semaphore()
    for k in range(1, FEAT):
        pl.semaphore_signal(barrier, inc=1, device_id=feat(k), device_id_type=MESH)
    for k in range(1, X):
        pl.semaphore_signal(barrier, inc=1, device_id=along_x(k), device_id_type=MESH)
    for k in DISTANCES:
        pl.semaphore_signal(barrier, inc=1, device_id=along_z(k), device_id_type=MESH)

    loads = [
        pltpu.make_async_copy(coords_hbm, coords_ref, sl.at[0]),
        pltpu.make_async_copy(map_hbm, map_ref, sl.at[1]),
        pltpu.make_async_copy(pairs_hbm, pairs_ref, sl.at[2]),
    ]
    for load in loads:
        load.start()
    for load in loads:
        load.wait()
    lane = lax.broadcasted_iota(I32, (1, BLOCKS), 1) - lax.rem(me, 8) * 16
    here = jnp.where((lane >= 0) & (lane < 16), -1, 0)
    for i in range(OWN):
        w = map_ref[0, i]
        place = (w // HALF) * (3 * HALF) + lax.rem(w, HALF)
        for k in range(3):
            here = jnp.where(lane == k * OWN + i, place + k * HALF, here)
    wide_ref[...] = jnp.zeros_like(wide_ref)
    for k in range(3):
        wide_ref[pl.ds(k * OWN, OWN), :] = coords_ref[k].astype(F32)
    wide_ref[12:13, :] = here.astype(F32)
    tile_ref[...] = wide_ref[...].astype(BF16)

    pl.semaphore_wait(barrier, FEAT - 1 + X - 1 + Z - 1)

    def tile_copy(k, slot):
        return pltpu.make_async_remote_copy(
            src_ref=tile_ref, dst_ref=y_ref.at[slot], send_sem=s1.at[k], recv_sem=r1.at[slot],
            device_id=feat(k), device_id_type=MESH)

    columns = pl.ds(pl.multiple_of(lax.rem(frame, 2) * COLS, COLS), COLS)

    def pair_copy(k):
        return pltpu.make_async_remote_copy(
            src_ref=pairs_ref.at[:, columns], dst_ref=cp_ref, send_sem=sp.at[k], recv_sem=rp,
            device_id=feat(k), device_id_type=MESH)

    for k in range(1, FEAT):
        tile_copy(k, me).start()

    @pl.when(me == owner)
    def _():
        for k in range(1, FEAT):
            pair_copy(k).start()
        cp_ref[...] = pairs_ref[:, columns]

    y_ref[me] = tile_ref[...]
    for j in range(ROWS // BLOCKS):
        part = pl.ds(j * BLOCKS, BLOCKS)
        left_pairs[part, :] = pair_matrix(pairs_ref[:, part]).T.astype(BF16)
    left_sum[...] = jnp.zeros_like(left_sum)
    right_sum[...] = jnp.zeros_like(right_sum)
    for k in range(1, FEAT):
        tile_copy(k, lax.rem(me + k, FEAT)).wait_recv()

    tiles = y_ref[...]
    low = jnp.sum(tiles[:8].astype(F32), axis=0)[12:13]
    high = jnp.sum(tiles[8:].astype(F32), axis=0)[12:13]
    places = jnp.concatenate([low, high], axis=1)
    ids = lax.broadcasted_iota(I32, (3 * REPLICAS, FEAT * 16), 0).astype(F32)
    match = (ids == places).astype(F32).astype(BF16)
    own = jnp.dot(match, tiles.reshape(FEAT * 16, BLOCKS), preferred_element_type=F32).astype(BF16)
    for h in range(C):
        g_ref[h, x, z] = own[h * 3 * HALF : (h + 1) * 3 * HALF]

    def z_send(k):
        return pltpu.make_async_remote_copy(
            src_ref=g_ref.at[c, x, z], dst_ref=g_ref.at[c, x, z], send_sem=sz.at[k % Z], recv_sem=rz.at[z],
            device_id=along_z(k), device_id_type=MESH)

    def z_arrival(zz):
        return pltpu.make_async_remote_copy(
            src_ref=g_ref.at[c, x, zz], dst_ref=g_ref.at[c, x, zz], send_sem=sz.at[0], recv_sem=rz.at[zz],
            device_id=along_z(1), device_id_type=MESH)

    def x_copy(k, xx, zz):
        return pltpu.make_async_remote_copy(
            src_ref=g_ref.at[c, xx, zz], dst_ref=g_ref.at[c, xx, zz], send_sem=sx.at[k, zz], recv_sem=rx.at[xx, zz],
            device_id=along_x(k), device_id_type=MESH)

    def core_copy(half, xx, zz):
        return pltpu.make_async_remote_copy(
            src_ref=g_ref.at[half, xx, zz], dst_ref=g_ref.at[half, xx, zz], send_sem=sc.at[xx, zz], recv_sem=rc.at[xx, zz],
            device_id={"core": 1 - c}, device_id_type=MESH)

    for k in DISTANCES:
        z_send(k).start()
    for k in (1, 3, 2):
        x_copy(k, x, z).start()

    @pl.when(me == owner)
    def _():
        for k in range(1, FEAT):
            pair_copy(k).wait_send()

    @pl.when(me != owner)
    def _():
        pair_copy(1).wait_recv()

    right_pairs[...] = pair_matrix(cp_ref[...]).astype(BF16)
    for k in DISTANCES:
        zz = lax.rem(z - k + Z, Z)
        z_arrival(zz).wait_recv()
        for kx in (1, 3, 2):
            x_copy(kx, x, zz).start()
        core_copy(c, x, zz).start()
    for k in DISTANCES:
        core_copy(1 - c, x, lax.rem(z - k + Z, Z)).wait_recv()

    def place_of(i):
        k = i // 2
        xx = lax.rem(x + k + (k // 2) * (5 - 2 * k), X)
        return xx, lax.rem(near + i, 2) * SPAN

    def group(i, carry):
        @pl.when((i >= 1) & (i < 2 * X - 1))
        def _():
            xx, first = place_of(i + 1)
            for j in range(SPAN):
                x_copy(1, xx, first + j).wait_recv()
                core_copy(c, xx, first + j).start()

        xx, first = place_of(i)

        @pl.when(i >= 2)
        def _():
            for j in range(SPAN):
                core_copy(1 - c, xx, first + j).wait_recv()

        comps = [
            jnp.concatenate(
                [g_ref[h, xx, first + j, k * HALF : (k + 1) * HALF, :] for j in range(SPAN) for h in range(C)], axis=0)
            for k in range(3)
        ]
        part = pl.ds(pl.multiple_of((xx * Z + first) * REPLICAS, GROUP), GROUP)
        total = None
        for comp in comps:
            d = lax.dot_general(left_pairs[...], comp, NT, preferred_element_type=F32)
            total = d * d if total is None else total + d * d
        f = root(total)
        left_ref[:, part] = f
        left_sum[...] += f[:, :128] + f[:, 128:]
        total = None
        for comp in comps:
            d = jnp.dot(comp, right_pairs[...], preferred_element_type=F32)
            total = d * d if total is None else total + d * d
        f = root(total)
        right_ref[part, :] = f
        right_sum[...] += jnp.sum(f.reshape(GROUP // 8, 8, COLS), axis=0)
        return carry

    lax.fori_loop(0, 2 * X, group, 0)

    for k in range(1, FEAT):
        tile_copy(k, me).wait_send()
    for k in DISTANCES:
        z_send(k).wait_send()
    for zz in range(Z):
        for k in range(1, X):
            x_copy(k, x, zz).wait_send()
    for k in DISTANCES:
        core_copy(c, x, lax.rem(z - k + Z, Z)).wait_send()
    for k in range(1, X):
        for zz in range(Z):
            core_copy(c, lax.rem(x + k, X), zz).wait_send()


def features(coords, walker_map, pairs):
    vmem = pl.BlockSpec(memory_space=pltpu.VMEM)
    hbm = pl.BlockSpec(memory_space=pltpu.HBM)
    dma = pltpu.SemaphoreType.DMA
    return pl.pallas_call(
        features_kernel,
        out_shape=(
            jax.ShapeDtypeStruct((ROWS, SAMPLES), F32),
            jax.ShapeDtypeStruct((SAMPLES, COLS), F32),
            jax.ShapeDtypeStruct((ROWS, 128), F32),
            jax.ShapeDtypeStruct((8, COLS), F32),
        ),
        in_specs=[hbm] * 3,
        out_specs=(vmem,) * 4,
        scratch_shapes=[
            pltpu.VMEM((3, OWN, BLOCKS), BF16),
            pltpu.SMEM((1, OWN), I32),
            pltpu.VMEM((2, ROWS), I32),
            pltpu.VMEM((16, BLOCKS), F32),
            pltpu.VMEM((16, BLOCKS), BF16),
            pltpu.VMEM((FEAT, 16, BLOCKS), BF16),
            pltpu.VMEM((2, COLS), I32),
            pltpu.VMEM((C, X, Z, 3 * HALF, BLOCKS), BF16),
            pltpu.VMEM((ROWS, BLOCKS), BF16),
            pltpu.VMEM((BLOCKS, COLS), BF16),
            dma((3,)), dma((FEAT,)), dma((FEAT,)), dma((FEAT,)), dma, dma((Z,)), dma((Z,)),
            dma((X, Z)), dma((X, Z)), dma((X, Z)), dma((X, Z)),
        ],
        compiler_params=pltpu.CompilerParams(collective_id=0, has_side_effects=True, vmem_limit_bytes=32 << 20),
        name="features",
    )(*(pltpu.with_memory_space_constraint(a, pltpu.HBM) for a in (jnp.transpose(coords[0], (1, 0, 2)), walker_map, pairs)))


def covariance_kernel(left_raw, right_raw, left_sum, right_sum, inst_ref, lag_ref, left, right, inst, lag, sem):
    left_mean = jnp.sum(left_sum[...], axis=1, keepdims=True) * (1.0 / SAMPLES)
    right_mean = jnp.sum(right_sum[...], axis=0, keepdims=True) * (1.0 / SAMPLES)
    for k in range(SAMPLES // GROUP):
        part = pl.ds(k * GROUP, GROUP)
        left[:, part] = (left_raw[:, part] - left_mean).astype(BF16)
        right[part, :] = (right_raw[part, :] - right_mean).astype(BF16)

    step = 256
    copies = []

    def put(values, buffer, target, rows):
        buffer[rows, :] = values
        copy = pltpu.make_async_copy(buffer.at[rows], target.at[rows], sem.at[len(copies)])
        copy.start()
        copies.append(copy)

    for k in range(ROWS // step):
        rows = pl.ds(k * step, step)
        total = jnp.dot(left[rows, :], right[...], preferred_element_type=F32)
        put(total * (1.0 / SAMPLES), inst, inst_ref, rows)
    for k in range(ROWS // step):
        rows = pl.ds(k * step, step)
        total = jnp.dot(left[rows, :PAIRED], right[LAG * REPLICAS :, :], preferred_element_type=F32)
        put(total * (1.0 / PAIRED), lag, lag_ref, rows)
    for copy in copies:
        copy.wait()


def covariances(left_raw, right_raw, left_sum, right_sum):
    vmem = pl.BlockSpec(memory_space=pltpu.VMEM)
    hbm = pl.BlockSpec(memory_space=pl.ANY)
    return pl.pallas_call(
        covariance_kernel,
        out_shape=(jax.ShapeDtypeStruct((ROWS, COLS), F32),) * 2,
        in_specs=[vmem] * 4,
        out_specs=(hbm, hbm),
        scratch_shapes=[
            pltpu.VMEM((ROWS, SAMPLES), BF16),
            pltpu.VMEM((SAMPLES, COLS), BF16),
            pltpu.VMEM((ROWS, COLS), F32),
            pltpu.VMEM((ROWS, COLS), F32),
            pltpu.SemaphoreType.DMA((8,)),
        ],
        compiler_params=pltpu.CompilerParams(vmem_limit_bytes=40 << 20),
        name="covariances",
    )(left_raw, right_raw, left_sum, right_sum)


def per_device(coords, walker_map, pairs):
    return covariances(*features(coords, walker_map, pairs))


def solution(mesh):
    split = Mesh(mesh.devices.reshape(X, Z, Y, C), ("x", "z", "y", "core"))
    frame, feat = ("x", "z"), ("y", "core")
    return jax.shard_map(
        per_device,
        mesh=split,
        in_specs=(P(frame, feat, None, None), P(frame, feat), P(None, feat)),
        out_specs=(P(feat, frame), P(feat, frame)),
        check_vma=False,
    )
```
